32 devices in a mesh: groups: 1, seq: 32 (over z, y, x, core).
Axes of the slice: x: 2, y: 2, z: 4, core: 2. Of those that a mesh axis runs over, the one named last changes fastest.
Arguments:
- queries: bfloat16 [4096, 4096], P(('groups', 'seq')), may hold values from -100 to 100
- keys_values: bfloat16 [4096, 2, 512], P(('groups', 'seq')), may hold values from -5 to 5
- head_signs: int32 [32, 128], replicated, may hold values from -1 to 1, as said below
- out_codes: int32 [512, 8192], P(None, 'seq'), may hold values from -2147483648 to 2147483647, as said below
- out_scales: bfloat16 [32, 8192], replicated, may hold values from 0.019897461 to 0.19921875
Outputs:
- projected: bfloat16 [4096, 8192], P(('groups', 'seq'))
The draws below stay inside these ranges and needn't reach their ends.
Inputs may be any that keep to these rules, and one draw needn't show every extreme that they name: `head_signs`: every entry is -1 or 1. `out_codes`: each word holds eight codes of 0 to 15, the code of row 8 i + k in bits 4k to 4k + 3 of word row i, the word read as a signed 32-bit integer.
All inputs are finite; a program needn't handle non-finite values.
Results may differ from the reference program's by a relative error of at most 0.006.
Values may be sent and summed in bfloat16 or wider, within the bound.
A program may use at most 128 MiB of HBM per device.

```python
import functools
import math
import jax
import jax.numpy as jnp
from jax import lax

D = 8192
HEADS = 32
KV = 4
HD = 128
GROUP = 128
WINDOW = 2048
TOKENS = 4096


def pair_draw(key):
    query_key = jax.random.fold_in(key, 101)
    kv_key = jax.random.fold_in(key, 102)
    base_queries = jnp.clip(jax.random.normal(query_key, (TOKENS, HEADS * HD), jnp.float32), -4.5, 4.5)
    base_kv = jnp.clip(jax.random.normal(kv_key, (TOKENS, 2, KV * HD), jnp.float32), -4.5, 4.5)
    return (base_queries, base_kv)


def draw_queries(key, part):
    return pair_draw(key)[0].astype(jnp.bfloat16)


def draw_keys_values(key, part):
    return pair_draw(key)[1].astype(jnp.bfloat16)


def draw_head_signs(key, part):
    sign_key = jax.random.fold_in(key, 301)
    return (2 * jax.random.randint(sign_key, (HEADS, HD), 0, 2, jnp.int32) - 1).astype(jnp.int32)


def draw_out_codes(key, part):
    code_key = jax.random.fold_in(key, 401)
    nibbles = jax.random.randint(code_key, (HEADS * HD // 8, D, 8), 0, 16, jnp.int32)
    shifted = [jnp.left_shift(nibbles[:, :, nibble_index], 4 * nibble_index) for nibble_index in range(8)]
    return functools.reduce(jnp.bitwise_or, shifted).astype(jnp.int32)


def setup_inputs(seed: int = 0, part: int = 0) -> dict:
    splits = jax.random.split(jax.random.key(seed), 6)
    part_keys = jax.random.split(jax.random.fold_in(splits[5], part), 6)
    return {
        "queries": draw_queries(jax.random.fold_in(jax.random.fold_in(splits[5], part), 71), part),
        "keys_values": draw_keys_values(jax.random.fold_in(jax.random.fold_in(splits[5], part), 71), part),
        "head_signs": draw_head_signs(jax.random.fold_in(splits[5], 71), part),
        "out_codes": draw_out_codes(jax.random.fold_in(splits[5], 71), part),
        "out_scales": jnp.clip(jnp.exp(jax.random.uniform(splits[4], (HEADS * HD // GROUP, D), jnp.float32, math.log(0.019897461), math.log(0.19921875))), 0.019897461, 0.19921875).astype(jnp.bfloat16),
    }


def hadamard(order):
    index = jnp.arange(order, dtype=jnp.int32)
    common = jnp.bitwise_and(index[:, None], index[None, :])
    ones = jnp.zeros((order, order), jnp.int32)
    for bit_index in range(order.bit_length()):
        ones = ones + jnp.bitwise_and(jnp.right_shift(common, bit_index), 1)
    return jnp.where(ones % 2 == 0, 1.0, -1.0).astype(jnp.float32)

def unpack(code_words):
    nibbles = [jnp.bitwise_and(jnp.right_shift(code_words, 4 * nibble_index), 15) for nibble_index in range(8)]
    stacked = jnp.stack(nibbles, axis=1)
    stacked = stacked.reshape(code_words.shape[0] * 8, code_words.shape[1])
    return (stacked - 8).astype(jnp.float32)

def rotate(attended, head_signs):
    signed = attended * head_signs.astype(jnp.float32)[None]
    mixed = jnp.einsum('thd,de->the', signed, hadamard(HD), precision=lax.Precision.HIGHEST) / math.sqrt(HD)
    return mixed.astype(jnp.bfloat16).reshape(attended.shape[0], HEADS * HD)

def reference(queries, keys_values, head_signs, out_codes, out_scales):
    per_group = HEADS // KV
    block_rows = math.gcd(TOKENS, 512)
    block_count = TOKENS // block_rows
    key_count = WINDOW + block_rows
    padded = jnp.concatenate([jnp.zeros((WINDOW, 2, KV * HD), keys_values.dtype), keys_values], axis=0)

    def attend(block):
        start = (block * block_rows).astype(jnp.int32)
        query_rows = lax.dynamic_slice_in_dim(queries, start, block_rows, 0).astype(jnp.float32)
        query_rows = query_rows.reshape(block_rows, KV, per_group, HD)
        key_value = lax.dynamic_slice_in_dim(padded, start, key_count, 0).astype(jnp.float32)
        key_rows = key_value[:, 0].reshape(key_count, KV, HD)
        value_rows = key_value[:, 1].reshape(key_count, KV, HD)
        scores = jnp.einsum('iGhd,jGd->Ghij', query_rows, key_rows) / math.sqrt(HD)
        query_pos = start + jnp.arange(block_rows, dtype=jnp.int32)
        key_pos = start - WINDOW + jnp.arange(key_count, dtype=jnp.int32)
        distance = query_pos[:, None] - key_pos[None, :]
        allowed = (distance >= 0) & (distance < WINDOW) & (key_pos[None, :] >= 0)
        allowed = allowed[None, None]
        scores = jnp.where(allowed, scores, -jnp.inf)
        row_max = lax.optimization_barrier(jnp.max(scores, axis=-1, keepdims=True))
        weights = jnp.where(allowed, jnp.exp(scores - row_max), 0.0)
        total = lax.optimization_barrier(jnp.sum(weights, axis=-1, keepdims=True))
        rounded = lax.optimization_barrier(weights.astype(jnp.bfloat16)).astype(jnp.float32)
        weighted = jnp.einsum('Ghij,jGd->Ghid', rounded, value_rows) / total
        return jnp.transpose(weighted, (2, 0, 1, 3)).reshape(block_rows, HEADS, HD)
    attended = lax.map(attend, jnp.arange(block_count, dtype=jnp.int32)).reshape(TOKENS, HEADS, HD)
    rotated = rotate(attended, head_signs)
    code_vals = unpack(out_codes)
    scaled = code_vals.reshape(HEADS * HD // GROUP, GROUP, D) * out_scales.astype(jnp.float32)[:, None, :]
    weight = scaled.reshape(HEADS * HD, D).astype(jnp.bfloat16)
    return jnp.dot(rotated, weight, preferred_element_type=jnp.float32).astype(jnp.bfloat16)
```

```python
import functools
import math

import jax
import jax.numpy as jnp
from jax import lax
from jax.experimental import pallas as pl
from jax.experimental.pallas import tpu as pltpu
from jax.sharding import PartitionSpec as P

HEADS = 32
KV = 4
HD = 128
GROUP = 128
WINDOW = 2048
PLANE = 8
STEPS = 8
PER_STEP = HEADS // STEPS
LOG2E = 1.4426950408889634
MESH = pl.DeviceIdType.MESH
BF16 = jnp.bfloat16
F32 = jnp.float32

TO_COLUMN, TO_X, TO_Y, PASS_Y, PASS_X, TO_CORE = 0, 1, 2, 3, 4, 5
KINDS = 9


def reordered_hadamard():
    column = jnp.arange(HD, dtype=jnp.int32)
    source = (column % 16) * 8 + column // 16
    common = jnp.bitwise_and(jnp.arange(HD, dtype=jnp.int32)[:, None], source[None, :])
    ones = jnp.zeros((HD, HD), jnp.int32)
    for bit in range(HD.bit_length()):
        ones = ones + jnp.bitwise_and(jnp.right_shift(common, bit), 1)
    return jnp.where(ones % 2 == 0, 1.0, -1.0).astype(BF16)


def kernel(
    n, reach,
    q_ref, kv_ref, sign_ref, had_ref, codes_ref, scales_ref, out_ref,
    kvbuf, cbuf, rot, bias, local_sem, kv_send, kv_recv, c_send, c_recv,
):
    rows = q_ref.shape[0]
    cols = codes_ref.shape[1]
    planes = n // PLANE
    back = -(-reach // PLANE)
    me = lax.axis_index("seq")
    z = me // PLANE
    p = me % PLANE
    core, x, y = p % 2, (p // 2) % 2, p // 4
    dx, dy, dc = 2 - 4 * x, 4 - 8 * y, 1 - 2 * core
    px, py, pd = p + dx, p + dy, p + dx + dy

    def column(d):
        return lax.rem(z + d, planes) * PLANE + p

    barrier = pltpu.get_barrier_semaphore()
    peers = [column(d) for d in range(1, planes)] + [me + dx, me + dy, me + dc]
    for peer in peers:
        pl.semaphore_signal(barrier, inc=1, device_id={"seq": peer}, device_id_type=MESH)
    own_kv = pltpu.make_async_copy(kv_ref, kvbuf.at[back * PLANE + p], local_sem.at[0])
    own_codes = pltpu.make_async_copy(codes_ref, cbuf.at[me], local_sem.at[1])
    own_kv.start()
    own_codes.start()

    class Item:
        def __init__(self, buf, base, send, recv):
            self.buf, self.base, self.send, self.recv = buf, base, send, recv
            self.half = buf.shape[1] // 2

        def move(self, kind, d, q, target, part=None, source=None, to=None):
            block = self.buf.at[self.base(d) + q]
            if part is not None:
                block = self.buf.at[self.base(d) + q, pl.ds(part * self.half, self.half)]
            return pltpu.make_async_remote_copy(
                src_ref=block if source is None else source,
                dst_ref=block,
                send_sem=self.send.at[kind, d],
                recv_sem=self.recv.at[kind, d],
                device_id={"seq": target},
                device_id_type=MESH,
            )

        def to_column(self, d, source):
            return self.move(TO_COLUMN, d, p, column(d), source=source)

        def to_x(self, d):
            return self.move(TO_X, d, p, me + dx)

        def to_y(self, d):
            return self.move(TO_Y, d, p, me + dy)

        def pass_y(self, d):
            return self.move(PASS_Y, d, px, me + dy, part=0)

        def pass_x(self, d):
            return self.move(PASS_X, d, py, me + dx, part=1)

        def to_core(self, d, which):
            return self.move(TO_CORE + which, d, (p, px, py, pd)[which], me + dc)

        def stage1(self, d):
            self.to_x(d).start()
            self.to_y(d).start()
            self.to_core(d, 0).start()

        def stage2(self, d):
            self.to_x(d).wait_recv()
            self.pass_y(d).start()
            self.to_core(d, 1).start()
            self.to_y(d).wait_recv()
            self.pass_x(d).start()
            self.to_core(d, 2).start()

        def stage3(self, d):
            self.pass_y(d).wait_recv()
            self.pass_x(d).wait_recv()
            self.to_core(d, 3).start()

        def stage4(self, d):
            for which in range(4):
                self.to_core(d, which).wait_recv()

        def sent(self, d):
            for copy in (self.to_x(d), self.to_y(d), self.pass_y(d), self.pass_x(d)):
                copy.wait_send()
            for which in range(4):
                self.to_core(d, which).wait_send()

    kv = Item(kvbuf, lambda d: (back - d) * PLANE, kv_send, kv_recv)
    codes = Item(cbuf, lambda d: lax.rem(z + planes - d, planes) * PLANE, c_send, c_recv)

    own_kv.wait()
    own_codes.wait()
    pl.semaphore_wait(barrier, len(peers))

    def kv_out(d):
        block = kvbuf.at[back * PLANE + p]
        return pltpu.make_async_remote_copy(
            src_ref=block, dst_ref=kvbuf.at[(back - d) * PLANE + p],
            send_sem=kv_send.at[TO_COLUMN, d], recv_sem=kv_recv.at[TO_COLUMN, d],
            device_id={"seq": column(d)}, device_id_type=MESH,
        )

    def codes_out(d):
        return pltpu.make_async_remote_copy(
            src_ref=cbuf.at[me], dst_ref=cbuf.at[me],
            send_sem=c_send.at[TO_COLUMN, d], recv_sem=c_recv.at[TO_COLUMN, d],
            device_id={"seq": column(d)}, device_id_type=MESH,
        )

    def there(d):
        return z - d >= 0

    near = [d for d in range(1, back + 1) if d < planes]
    for d in near:
        @pl.when(z + d < planes)
        def _():
            kv_out(d).start()
    kv.stage1(0)
    for d in range(1, planes):
        codes_out(d).start()

    for d in range(1, back + 1):
        @pl.when(jnp.logical_not(there(d)))
        def _():
            first = (back - d) * PLANE
            kvbuf[first:first + PLANE] = jnp.zeros((PLANE,) + kvbuf.shape[1:], kvbuf.dtype)

    window_blocks = reach + 1
    first_block = back * PLANE + p - reach
    keys = window_blocks * rows
    query = lax.broadcasted_iota(jnp.int32, (rows, keys), 0)
    key = lax.broadcasted_iota(jnp.int32, (rows, keys), 1) - reach * rows
    gap = query - key
    allowed = (gap >= 0) & (gap < WINDOW) & (key + me * rows >= 0)
    bias[...] = jnp.where(allowed, 0.0, -jnp.inf).astype(F32)

    for d in range(0, back + 1):
        if d in near:
            @pl.when(there(d))
            def _():
                kv_out(d).wait_recv()
                kv.stage1(d)
        if d >= 1 and (d == 1 or d - 1 in near):
            @pl.when(there(d - 1))
            def _():
                kv.stage2(d - 1)
    levels = [0] + near
    @pl.when(there(levels[-1]))
    def _():
        kv.stage2(levels[-1])
    codes.stage1(0)
    for d in levels:
        @pl.when(there(d))
        def _():
            kv.stage3(d)
    for d in levels:
        @pl.when(there(d))
        def _():
            kv.stage4(d)

    def event(j):
        @pl.when(j < planes)
        def _():
            codes_out(j).wait_recv()
            codes.stage1(j)

        @pl.when(j - 1 < planes)
        def _():
            codes.stage2(j - 1)

    def third(d):
        @pl.when(d < planes)
        def _():
            codes.stage3(d)

    def attend(t, carry):
        start = pl.multiple_of(t * (PER_STEP * HD), PER_STEP * HD)
        group = (t * PER_STEP) // (HEADS // KV)
        q = q_ref[:, pl.ds(start, PER_STEP * HD)]
        q = jnp.concatenate([q[:, k * HD:(k + 1) * HD] for k in range(PER_STEP)], axis=0)
        key_lane = pl.multiple_of(group * HD, HD)
        value_lane = pl.multiple_of(group * HD + KV * HD, HD)
        k_rows = kvbuf[pl.ds(first_block, window_blocks), :, pl.ds(key_lane, HD)].reshape(keys, HD)
        v_rows = kvbuf[pl.ds(first_block, window_blocks), :, pl.ds(value_lane, HD)].reshape(keys, HD)
        scores = lax.dot_general(q, k_rows, (((1,), (1,)), ((), ())), preferred_element_type=F32)
        scores = scores.reshape(PER_STEP, rows, keys) * (LOG2E / math.sqrt(HD)) + bias[...][None]
        top = jnp.max(scores, axis=-1, keepdims=True)
        weights = jnp.exp2(scores - top)
        total = jnp.sum(weights, axis=-1, keepdims=True)
        rounded = weights.astype(BF16).reshape(PER_STEP * rows, keys)
        weighted = jnp.dot(rounded, v_rows, preferred_element_type=F32)
        weighted = weighted.reshape(PER_STEP, rows, HD) / total
        signed = weighted * sign_ref[t].astype(F32)[:, None, :]
        signed = signed.reshape(PER_STEP * rows, HD)
        high = signed.astype(BF16)
        low = (signed - high.astype(F32)).astype(BF16)
        mixed = jnp.dot(high, had_ref[...], preferred_element_type=F32)
        mixed = mixed + jnp.dot(low, had_ref[...], preferred_element_type=F32)
        mixed = (mixed * (1.0 / math.sqrt(HD))).astype(BF16)
        for k in range(PER_STEP):
            lanes = pl.ds(pl.multiple_of(start + k * HD, HD), HD)
            rot[:, lanes] = mixed[k * rows:(k + 1) * rows]

        @pl.when(t == 2)
        def _():
            event(1)

        @pl.when(t == 5)
        def _():
            event(2)
            third(0)

        return carry

    lax.fori_loop(0, STEPS, attend, 0)

    chunk_heads = 8
    words = GROUP // 8

    def project(s):
        lanes = pl.ds(pl.multiple_of(s * cols, cols), cols)
        scale = scales_ref[:, lanes]
        acc = jnp.zeros((rows, cols), F32)
        for chunk in range(HEADS // chunk_heads):
            parts = []
            for h in range(chunk * chunk_heads, (chunk + 1) * chunk_heads):
                word = cbuf[s, h * words:(h + 1) * words, :] ^ jnp.int32(-2004318072)
                factor = jnp.broadcast_to(scale[h:h + 1, :], (words, cols))
                for k in range(8):
                    code = jnp.right_shift(jnp.left_shift(word, 28 - 4 * k), 28)
                    parts.append(code.astype(F32).astype(BF16) * factor)
            weight = jnp.concatenate(parts, axis=0)
            piece = rot[:, chunk * chunk_heads * HD:(chunk + 1) * chunk_heads * HD]
            acc = acc + jnp.dot(piece, weight, preferred_element_type=F32)
        out_ref[:, lanes] = acc.astype(BF16)

    def finish(j, carry):
        event(j)
        third(j - 2)
        level = j - 3
        codes.stage4(level)
        base = codes.base(level)

        def one(q, c):
            project(base + q)
            return c

        return lax.fori_loop(0, PLANE, one, carry)

    lax.fori_loop(3, planes + 3, finish, 0)

    for d in near:
        @pl.when(z + d < planes)
        def _():
            kv_out(d).wait_send()
    for d in levels:
        @pl.when(there(d))
        def _():
            kv.sent(d)
    for d in range(1, planes):
        codes_out(d).wait_send()

    def sent(d, carry):
        codes.sent(d)
        return carry

    lax.fori_loop(0, planes, sent, 0)


def on_device(queries, keys_values, head_signs, out_codes, out_scales):
    n = lax.axis_size("seq")
    rows = queries.shape[0]
    reach = (WINDOW + rows - 2) // rows
    back = -(-reach // PLANE)
    planes = n // PLANE
    word_rows, cols = out_codes.shape
    vmem = pl.BlockSpec(memory_space=pltpu.VMEM)
    dma = pltpu.SemaphoreType.DMA
    return pl.pallas_call(
        functools.partial(kernel, n, reach),
        out_shape=jax.ShapeDtypeStruct((rows, n * cols), BF16),
        in_specs=[vmem] * 6,
        out_specs=vmem,
        scratch_shapes=[
            pltpu.VMEM(((back + 1) * PLANE, rows, 2 * KV * HD), BF16),
            pltpu.VMEM((n, word_rows, cols), jnp.int32),
            pltpu.VMEM((rows, HEADS * HD), BF16),
            pltpu.VMEM((rows, (reach + 1) * rows), F32),
            dma((2,)),
            dma((KINDS, back + 1)),
            dma((KINDS, back + 1)),
            dma((KINDS, planes)),
            dma((KINDS, planes)),
        ],
        compiler_params=pltpu.CompilerParams(
            collective_id=0, has_side_effects=True, vmem_limit_bytes=64 * 1000 * 1000
        ),
    )(
        queries,
        keys_values.reshape(rows, 2 * KV * HD),
        head_signs.reshape(STEPS, PER_STEP, HD),
        reordered_hadamard(),
        out_codes,
        out_scales,
    )


def solution(mesh):
    return jax.shard_map(
        on_device,
        mesh=mesh,
        in_specs=(
            P(("groups", "seq"), None),
            P(("groups", "seq"), None, None),
            P(),
            P(None, "seq"),
            P(),
        ),
        out_specs=P(("groups", "seq"), None),
        check_vma=False,
    )
```

```python
import functools
import math

import jax
import jax.numpy as jnp
from jax import lax
from jax.experimental import pallas as pl
from jax.experimental.pallas import tpu as pltpu
from jax.sharding import PartitionSpec as P

HEADS = 32
KV = 4
HD = 128
GROUP = 128
WINDOW = 2048
PLANE = 8
STEPS = 8
PER_STEP = HEADS // STEPS
LOG2E = 1.4426950408889634
MESH = pl.DeviceIdType.MESH
BF16 = jnp.bfloat16
F32 = jnp.float32

TO_COLUMN, TO_X, TO_Y, PASS_Y, PASS_X, TO_CORE = 0, 1, 2, 3, 4, 5
KINDS = 9


def reordered_hadamard():
    column = jnp.arange(HD, dtype=jnp.int32)
    source = (column % 16) * 8 + column // 16
    common = jnp.bitwise_and(jnp.arange(HD, dtype=jnp.int32)[:, None], source[None, :])
    ones = jnp.zeros((HD, HD), jnp.int32)
    for bit in range(HD.bit_length()):
        ones = ones + jnp.bitwise_and(jnp.right_shift(common, bit), 1)
    return jnp.where(ones % 2 == 0, 1.0, -1.0).astype(BF16)


def kernel(
    n, reach,
    q_ref, kv_ref, sign_ref, had_ref, codes_ref, scales_ref, out_ref,
    kvbuf, cbuf, rot, bias, local_sem, kv_send, kv_recv, c_send, c_recv,
):
    rows = q_ref.shape[0]
    cols = codes_ref.shape[1]
    planes = n // PLANE
    back = -(-reach // PLANE)
    me = lax.axis_index("seq")
    z = me // PLANE
    p = me % PLANE
    core, x, y = p % 2, (p // 2) % 2, p // 4
    dx, dy, dc = 2 - 4 * x, 4 - 8 * y, 1 - 2 * core
    px, py, pd = p + dx, p + dy, p + dx + dy

    def column(d):
        return lax.rem(z + d, planes) * PLANE + p

    barrier = pltpu.get_barrier_semaphore()
    peers = [column(d) for d in range(1, planes)] + [me + dx, me + dy, me + dc]
    for peer in peers:
        pl.semaphore_signal(barrier, inc=1, device_id={"seq": peer}, device_id_type=MESH)
    own_kv = pltpu.make_async_copy(kv_ref, kvbuf.at[back * PLANE + p], local_sem.at[0])
    own_codes = pltpu.make_async_copy(codes_ref, cbuf.at[me], local_sem.at[1])
    own_kv.start()
    own_codes.start()

    class Item:
        def __init__(self, buf, base, send, recv):
            self.buf, self.base, self.send, self.recv = buf, base, send, recv
            self.half = buf.shape[1] // 2

        def move(self, kind, d, q, target, part=None, source=None, to=None):
            block = self.buf.at[self.base(d) + q]
            if part is not None:
                block = self.buf.at[self.base(d) + q, pl.ds(part * self.half, self.half)]
            return pltpu.make_async_remote_copy(
                src_ref=block if source is None else source,
                dst_ref=block,
                send_sem=self.send.at[kind, d],
                recv_sem=self.recv.at[kind, d],
                device_id={"seq": target},
                device_id_type=MESH,
            )

        def to_column(self, d, source):
            return self.move(TO_COLUMN, d, p, column(d), source=source)

        def to_x(self, d):
            return self.move(TO_X, d, p, me + dx)

        def to_y(self, d):
            return self.move(TO_Y, d, p, me + dy)

        def pass_y(self, d):
            return self.move(PASS_Y, d, px, me + dy, part=0)

        def pass_x(self, d):
            return self.move(PASS_X, d, py, me + dx, part=1)

        def to_core(self, d, which):
            return self.move(TO_CORE + which, d, (p, px, py, pd)[which], me + dc)

        def stage1(self, d):
            self.to_x(d).start()
            self.to_y(d).start()
            self.to_core(d, 0).start()

        def stage2(self, d):
            self.to_x(d).wait_recv()
            self.pass_y(d).start()
            self.to_core(d, 1).start()
            self.to_y(d).wait_recv()
            self.pass_x(d).start()
            self.to_core(d, 2).start()

        def stage3(self, d):
            self.pass_y(d).wait_recv()
            self.pass_x(d).wait_recv()
            self.to_core(d, 3).start()

        def stage4(self, d):
            for which in range(4):
                self.to_core(d, which).wait_recv()

        def sent(self, d):
            for copy in (self.to_x(d), self.to_y(d), self.pass_y(d), self.pass_x(d)):
                copy.wait_send()
            for which in range(4):
                self.to_core(d, which).wait_send()

    kv = Item(kvbuf, lambda d: (back - d) * PLANE, kv_send, kv_recv)
    codes = Item(cbuf, lambda d: lax.rem(z + planes - d, planes) * PLANE, c_send, c_recv)

    own_kv.wait()
    own_codes.wait()
    pl.semaphore_wait(barrier, len(peers))

    def kv_out(d):
        block = kvbuf.at[back * PLANE + p]
        return pltpu.make_async_remote_copy(
            src_ref=block, dst_ref=kvbuf.at[(back - d) * PLANE + p],
            send_sem=kv_send.at[TO_COLUMN, d], recv_sem=kv_recv.at[TO_COLUMN, d],
            device_id={"seq": column(d)}, device_id_type=MESH,
        )

    def codes_out(d):
        return pltpu.make_async_remote_copy(
            src_ref=cbuf.at[me], dst_ref=cbuf.at[me],
            send_sem=c_send.at[TO_COLUMN, d], recv_sem=c_recv.at[TO_COLUMN, d],
            device_id={"seq": column(d)}, device_id_type=MESH,
        )

    def there(d):
        return z - d >= 0

    near = [d for d in range(1, back + 1) if d < planes]
    for d in near:
        @pl.when(z + d < planes)
        def _():
            kv_out(d).start()
    kv.stage1(0)
    for d in range(1, planes):
        codes_out(d).start()

    for d in range(1, back + 1):
        @pl.when(jnp.logical_not(there(d)))
        def _():
            first = (back - d) * PLANE
            kvbuf[first:first + PLANE] = jnp.zeros((PLANE,) + kvbuf.shape[1:], kvbuf.dtype)

    window_blocks = reach + 1
    first_block = back * PLANE + p - reach
    keys = window_blocks * rows
    query = lax.broadcasted_iota(jnp.int32, (rows, keys), 0)
    key = lax.broadcasted_iota(jnp.int32, (rows, keys), 1) - reach * rows
    gap = query - key
    allowed = (gap >= 0) & (gap < WINDOW) & (key + me * rows >= 0)
    bias[...] = jnp.where(allowed, 0.0, -jnp.inf).astype(F32)

    for d in range(0, back + 1):
        if d in near:
            @pl.when(there(d))
            def _():
                kv_out(d).wait_recv()
                kv.stage1(d)
        if d >= 1 and (d == 1 or d - 1 in near):
            @pl.when(there(d - 1))
            def _():
                kv.stage2(d - 1)
    levels = [0] + near
    @pl.when(there(levels[-1]))
    def _():
        kv.stage2(levels[-1])
    codes.stage1(0)
    for d in levels:
        @pl.when(there(d))
        def _():
            kv.stage3(d)
    for d in levels:
        @pl.when(there(d))
        def _():
            kv.stage4(d)

    def event(j):
        @pl.when(j < planes)
        def _():
            codes_out(j).wait_recv()
            codes.stage1(j)

        @pl.when(j - 1 < planes)
        def _():
            codes.stage2(j - 1)

    def third(d):
        @pl.when(d < planes)
        def _():
            codes.stage3(d)

    def attend(t, carry):
        start = pl.multiple_of(t * (PER_STEP * HD), PER_STEP * HD)
        group = (t * PER_STEP) // (HEADS // KV)
        q = q_ref[:, pl.ds(start, PER_STEP * HD)]
        q = jnp.concatenate([q[:, k * HD:(k + 1) * HD] for k in range(PER_STEP)], axis=0)
        key_lane = pl.multiple_of(group * HD, HD)
        value_lane = pl.multiple_of(group * HD + KV * HD, HD)
        k_rows = kvbuf[pl.ds(first_block, window_blocks), :, pl.ds(key_lane, HD)].reshape(keys, HD)
        v_rows = kvbuf[pl.ds(first_block, window_blocks), :, pl.ds(value_lane, HD)].reshape(keys, HD)
        scores = lax.dot_general(q, k_rows, (((1,), (1,)), ((), ())), preferred_element_type=F32)
        scores = scores.reshape(PER_STEP, rows, keys) * (LOG2E / math.sqrt(HD)) + bias[...][None]
        top = jnp.max(scores, axis=-1, keepdims=True)
        weights = jnp.exp2(scores - top)
        total = jnp.sum(weights, axis=-1, keepdims=True)
        rounded = weights.astype(BF16).reshape(PER_STEP * rows, keys)
        weighted = jnp.dot(rounded, v_rows, preferred_element_type=F32)
        weighted = weighted.reshape(PER_STEP, rows, HD) / total
        signed = weighted * sign_ref[t].astype(F32)[:, None, :]
        signed = signed.reshape(PER_STEP * rows, HD)
        high = signed.astype(BF16)
        low = (signed - high.astype(F32)).astype(BF16)
        mixed = jnp.dot(high, had_ref[...], preferred_element_type=F32)
        mixed = mixed + jnp.dot(low, had_ref[...], preferred_element_type=F32)
        mixed = (mixed * (1.0 / math.sqrt(HD))).astype(BF16)
        for k in range(PER_STEP):
            lanes = pl.ds(pl.multiple_of(start + k * HD, HD), HD)
            rot[:, lanes] = mixed[k * rows:(k + 1) * rows]

        @pl.when(t == 2)
        def _():
            event(1)

        @pl.when(t == 5)
        def _():
            event(2)
            third(0)

        return carry

    lax.fori_loop(0, STEPS, attend, 0)

    chunk_heads = 8
    words = GROUP // 8

    def project(s):
        lanes = pl.ds(pl.multiple_of(s * cols, cols), cols)
        scale = scales_ref[:, lanes]
        acc = jnp.zeros((rows, cols), F32)
        for chunk in range(HEADS // chunk_heads):
            parts = []
            for h in range(chunk * chunk_heads, (chunk + 1) * chunk_heads):
                word = cbuf[s, h * words:(h + 1) * words, :] ^ jnp.int32(-2004318072)
                factor = jnp.broadcast_to(scale[h:h + 1, :], (words, cols))
                for k in range(8):
                    code = jnp.right_shift(jnp.left_shift(word, 28 - 4 * k), 28)
                    parts.append(code.astype(F32).astype(BF16) * factor)
            weight = jnp.concatenate(parts, axis=0)
            piece = rot[:, chunk * chunk_heads * HD:(chunk + 1) * chunk_heads * HD]
            acc = acc + jnp.dot(piece, weight, preferred_element_type=F32)
        out_ref[:, lanes] = acc.astype(BF16)

    def project_some(d, low, high):
        def one(q, c):
            which = q // 2
            project(codes.base(d) + p + (which % 2) * dx + (which // 2) * dy + (q % 2) * dc)
            return c

        lax.fori_loop(low, high, one, 0)

    def finish(j, carry):
        @pl.when(j - 3 < planes)
        def _():
            for which in range(3):
                codes.to_core(j - 3, which).wait_recv()
            project_some(j - 3, 0, 6)

        event(j)

        @pl.when(j >= 4)
        def _():
            third(j - 3)
            codes.to_core(j - 4, 3).wait_recv()
            project_some(j - 4, 6, 8)

        return carry

    lax.fori_loop(3, planes + 4, finish, 0)

    for d in near:
        @pl.when(z + d < planes)
        def _():
            kv_out(d).wait_send()
    for d in levels:
        @pl.when(there(d))
        def _():
            kv.sent(d)
    for d in range(1, planes):
        codes_out(d).wait_send()

    def sent(d, carry):
        codes.sent(d)
        return carry

    lax.fori_loop(0, planes, sent, 0)


def on_device(queries, keys_values, head_signs, out_codes, out_scales):
    n = lax.axis_size("seq")
    rows = queries.shape[0]
    reach = (WINDOW + rows - 2) // rows
    back = -(-reach // PLANE)
    planes = n // PLANE
    word_rows, cols = out_codes.shape
    vmem = pl.BlockSpec(memory_space=pltpu.VMEM)
    dma = pltpu.SemaphoreType.DMA
    return pl.pallas_call(
        functools.partial(kernel, n, reach),
        out_shape=jax.ShapeDtypeStruct((rows, n * cols), BF16),
        in_specs=[vmem] * 6,
        out_specs=vmem,
        scratch_shapes=[
            pltpu.VMEM(((back + 1) * PLANE, rows, 2 * KV * HD), BF16),
            pltpu.VMEM((n, word_rows, cols), jnp.int32),
            pltpu.VMEM((rows, HEADS * HD), BF16),
            pltpu.VMEM((rows, (reach + 1) * rows), F32),
            dma((2,)),
            dma((KINDS, back + 1)),
            dma((KINDS, back + 1)),
            dma((KINDS, planes)),
            dma((KINDS, planes)),
        ],
        compiler_params=pltpu.CompilerParams(
            collective_id=0, has_side_effects=True, vmem_limit_bytes=64 * 1000 * 1000
        ),
    )(
        queries,
        keys_values.reshape(rows, 2 * KV * HD),
        head_signs.reshape(STEPS, PER_STEP, HD),
        reordered_hadamard(),
        out_codes,
        out_scales,
    )


def solution(mesh):
    return jax.shard_map(
        on_device,
        mesh=mesh,
        in_specs=(
            P(("groups", "seq"), None),
            P(("groups", "seq"), None, None),
            P(),
            P(None, "seq"),
            P(),
        ),
        out_specs=P(("groups", "seq"), None),
        check_vma=False,
    )
```
